512 devices in a mesh: orb: 64 (over z, y), pair: 8 (over x, core).
Axes of the slice: x: 4, y: 8, z: 8, core: 2. Of those that a mesh axis runs over, the one named last changes fastest.
Arguments:
- amplitudes: bfloat16 [4096, 128, 128], P(('orb', 'pair')), may hold values from -6 to 6
- exchange_ints: bfloat16 [4096, 128, 128], P(('orb', 'pair')), may hold values from -6 to 6
- fock_off: bfloat16 [4096, 128, 128], P(('orb', 'pair')), may hold values from -0.6 to 0.6, as said below
- orbital_energies: float32 [4096, 128], P(('orb', 'pair')), may hold values from 0.5 to 4
- occ_shift: float32 [4096], P(('orb', 'pair')), may hold values from 0.5 to 1.5
- far_margins: bfloat16 [32768, 128, 128], P(('orb', 'pair')), may hold values from -0.5 to 0.5
- far_group: int32 [32768, 1], P(('orb', 'pair')), may hold values from 0 to 63; in each aligned block of 64 rows (0 to 63, 64 to 127, ...) at most 2 rows name the same one
- far_pair: int32 [32768], P(('orb', 'pair')), may hold values from 0 to 7
- far_target: int32 [32768], P(('orb', 'pair')), may hold values from 0 to 7
- near_margins: bfloat16 [8192, 128, 128], P(('orb', 'pair')), may hold values from -0.5 to 0.5
- near_column: int32 [8192, 1], P(('orb', 'pair')), may hold values from 0 to 7; in each aligned block of 16 rows (0 to 15, 16 to 31, ...) at most 4 rows name the same one
- near_pair: int32 [8192], P(('orb', 'pair')), may hold values from 0 to 7
- near_target: int32 [8192], P(('orb', 'pair')), may hold values from 0 to 7
Outputs:
- amplitudes_out: float32 [4096, 128, 128], P(('orb', 'pair'))
The draws below stay inside these ranges and needn't reach their ends.
Inputs may be any that keep to these rules, and one draw needn't show every extreme that they name: `far_group`: among the 64 blocks of one device at most 2 name the same group, and in every draw some device's blocks name some group exactly 2 times. `near_column`: among the 16 blocks of one device at most 4 name the same column, and in every draw some device's blocks name some column exactly 4 times. `fock_off`: each pair's matrix is symmetric with a zero diagonal.
All inputs are finite; a program needn't handle non-finite values.
Results may differ from the reference program's by a relative error of at most 0.0061.
Values may be sent and summed in bfloat16 or wider, within the bound.
A program may use at most 64 MiB of HBM per device.

```python
import math
import jax
import jax.numpy as jnp
import numpy as np
from jax import lax

P_SIZE = 128
PAIR_DEV = 8
BLK_O = 64
BLK_G = 16
ITERS = 2
NPAIRS = 4096
NBLK_O = 32768
NBLK_G = 8192
N_ORB = 64
N_PAIR = 8


def draw_fock_off(key, part):
    raw = jax.random.normal(key, (NPAIRS, P_SIZE, P_SIZE), jnp.float32)
    symmetric = (raw + jnp.swapaxes(raw, 1, 2)) * 0.70710678
    offdiag = 1.0 - jnp.eye(P_SIZE, dtype=jnp.float32)
    values = jnp.clip(symmetric * offdiag[None, :, :] / jnp.sqrt(jnp.float32(P_SIZE)), -0.59375, 0.59375)
    return values.astype(jnp.bfloat16)


def plant(values, own_key, smallest, top_value):
    longest = values.shape.index(max(values.shape))
    spots = []
    for shift in (0, 1):
        where = [jax.random.randint(jax.random.fold_in(own_key, axis), (), 0, length) for axis, length in enumerate(values.shape)]
        where[longest] = (where[longest] + shift) % values.shape[longest]
        spots.append(tuple(where))
    return values.at[spots[0]].set(smallest).at[spots[1]].set(top_value)


def block_levels(rng, shape, split, smallest, high):
    def one(axis_at, shards_of):
        draws = jax.random.uniform(jax.random.fold_in(jax.random.fold_in(rng, 6), axis_at), (shards_of,), jnp.float32, smallest / len(split), high / len(split))
        return jnp.repeat(jnp.exp(draws), shape[axis_at] // shards_of).reshape((-1,) + (1,) * (len(shape) - axis_at - 1))

    loudness = one(*split[0])
    for cut in split[1:]:
        loudness = loudness * one(*cut)
    return loudness


def routed_block(own_key, own, number, rows, amount, top, most, slope):
    ranking = jax.random.permutation(own_key, amount)
    heavy_load, common = shares(amount, rows * top, most, slope, True), shares(amount, rows * top, most, slope, False)
    places = jnp.arange(amount)

    def named(sizes, offset_by):
        used = int((sizes > 0).sum())
        fixed = max(1, used // 4)
        passed = fixed + (places - fixed + offset_by * (used - fixed)) % max(1, amount - fixed)
        return jnp.zeros((amount,), jnp.int32).at[ranking[jnp.where(places < fixed, places, passed)]].set(jnp.asarray(sizes, jnp.int32))

    sizes = jnp.where(number % 4 == 0, named(heavy_load, number // 4), named(common, number - number // 4 - 1))
    mixed = jax.random.permutation(jax.random.fold_in(own, 3), amount)
    donor, receiver = mixed[0:amount // 2 * 2:2], mixed[1:amount // 2 * 2:2]
    slack = jnp.minimum(sizes[donor] - 1, most - sizes[receiver]) // 2
    slack = jnp.where((donor == ranking[0]) | (receiver == ranking[0]) | (sizes[receiver] == 0), 0, jnp.maximum(slack, 0))
    passed = jax.random.randint(jax.random.fold_in(own, 4), (amount // 2,), 0, 1 << 20) % (slack + 1)
    sizes = sizes.at[donor].add(-passed).at[receiver].add(passed)
    members = jnp.searchsorted(jnp.cumsum(sizes), jnp.arange(rows * top), side="right").astype(jnp.int32)
    table = members.reshape(top, rows).T
    table = table[jax.random.permutation(jax.random.fold_in(own, 1), rows)]
    offset_by = jax.random.randint(jax.random.fold_in(own, 2), (rows, 1), 0, top)
    return jnp.take_along_axis(table, (jnp.arange(top)[None, :] + offset_by) % top, axis=1)


def shares(count, total, most, skew, full):
    loads = [(1 << 20) // math.isqrt(standing ** skew) + 1 for standing in range(1, count + 1)]
    largest = most if full else min(most, max(-(-total // count), total * loads[0] // sum(loads)))
    least = 1 if total - largest >= count - 1 else 0
    holding, surplus = [largest] + [least] * (count - 1), total - largest - least * (count - 1)
    while surplus > 0:
        movable = [i for i in range(1, count) if holding[i] < largest] or [i for i in range(1, count) if holding[i] < most]
        pool, budget = sum([loads[i] for i in movable]), surplus
        for i in movable:
            extra = min(most - holding[i], max(1, budget * loads[i] // pool), surplus)
            holding[i] = holding[i] + extra
            surplus = surplus - extra
    return np.array(holding)


def gaussian(own_key, shape, width, reach, pieces=(), kind=jnp.bfloat16):
    factor_of = block_levels(own_key, shape, pieces, -0.22, 0.18) if pieces else 1.0
    entries = jax.random.normal(own_key, shape, jnp.float32) * width * factor_of
    return jnp.minimum(jnp.maximum(entries, -reach), reach).astype(kind)


def setup_inputs(seed: int = 0) -> dict:
    seeds = jax.random.split(jax.random.key(seed), 14)
    amplitudes = gaussian(seeds[0], (NPAIRS, P_SIZE, P_SIZE), 1.0, 6.0, ((0, 512),))
    exchange_ints = gaussian(seeds[1], (NPAIRS, P_SIZE, P_SIZE), 1.0, 6.0, ((0, 512),))
    fock_off = draw_fock_off(jax.random.fold_in(seeds[13], 71), 0)
    orbital_energies = jnp.clip(jnp.exp(math.log(4.0) - 2.0794415 * jax.random.uniform(seeds[3], (NPAIRS, P_SIZE), jnp.float32) ** block_levels(seeds[3], (NPAIRS, P_SIZE), ((0, 512),), -0.2, 0.2)), 0.5, 4.0)
    occ_shift = jnp.clip(0.5 + 1.0 * jax.random.uniform(seeds[4], (NPAIRS,), jnp.float32) ** block_levels(seeds[4], (NPAIRS,), ((0, 512),), -0.2, 0.2), 0.5, 1.5)
    far_margins = gaussian(seeds[5], (NBLK_O, P_SIZE, P_SIZE), P_SIZE ** -0.5, 0.5, ((0, 512),))
    far_group_keys = jax.random.split(jax.random.fold_in(seeds[6], 1), NBLK_O // BLK_O)
    far_group_turns = jax.random.permutation(jax.random.fold_in(seeds[6], 3), NBLK_O // BLK_O)
    far_group = jax.vmap(lambda own, number: routed_block(jax.random.fold_in(seeds[6], 2), own, number, BLK_O, N_ORB, 1, 2 * BLK_O // N_ORB, 2))(far_group_keys, far_group_turns).reshape((NBLK_O, 1))
    far_pair = plant(jax.random.randint(seeds[7], (NBLK_O,), 0, PAIR_DEV), jax.random.fold_in(seeds[7], 1), 0, PAIR_DEV - 1).astype(jnp.int32)
    far_target = plant(jax.random.randint(seeds[8], (NBLK_O,), 0, PAIR_DEV), jax.random.fold_in(seeds[8], 1), 0, PAIR_DEV - 1).astype(jnp.int32)
    near_margins = gaussian(seeds[9], (NBLK_G, P_SIZE, P_SIZE), P_SIZE ** -0.5, 0.5, ((0, 512),))
    near_column_keys = jax.random.split(jax.random.fold_in(seeds[10], 1), NBLK_G // BLK_G)
    near_column_turns = jax.random.permutation(jax.random.fold_in(seeds[10], 3), NBLK_G // BLK_G)
    near_column = jax.vmap(lambda own, number: routed_block(jax.random.fold_in(seeds[10], 2), own, number, BLK_G, N_PAIR, 1, 2 * BLK_G // N_PAIR, 2))(near_column_keys, near_column_turns).reshape((NBLK_G, 1))
    near_pair = plant(jax.random.randint(seeds[11], (NBLK_G,), 0, PAIR_DEV), jax.random.fold_in(seeds[11], 1), 0, PAIR_DEV - 1).astype(jnp.int32)
    near_target = plant(jax.random.randint(seeds[12], (NBLK_G,), 0, PAIR_DEV), jax.random.fold_in(seeds[12], 1), 0, PAIR_DEV - 1).astype(jnp.int32)
    return dict(amplitudes=amplitudes, exchange_ints=exchange_ints, fock_off=fock_off, orbital_energies=orbital_energies, occ_shift=occ_shift, far_margins=far_margins, far_group=far_group, far_pair=far_pair, far_target=far_target, near_margins=near_margins, near_column=near_column, near_pair=near_pair, near_target=near_target)


def batched(left, right, form):
    return jnp.einsum(form, left.astype(jnp.float32), right.astype(jnp.float32))


def reference(amplitudes, exchange_ints, fock_off, orbital_energies, occ_shift, far_margins, far_group, far_pair, far_target, near_margins, near_column, near_pair, near_target):
    devices_all = N_ORB * N_PAIR
    denominator = orbital_energies[:, :, None] + orbital_energies[:, None, :] + occ_shift[:, None, None]
    current = amplitudes.astype(jnp.float32)
    device_numbers = jnp.arange(devices_all, dtype=jnp.int32)
    orbital_group = device_numbers // N_PAIR
    column_number = device_numbers % N_PAIR
    far_source = (far_group[:, 0].reshape(devices_all, BLK_O) * N_PAIR + column_number[:, None]) * PAIR_DEV + far_pair.reshape(devices_all, BLK_O)
    near_source = (orbital_group[:, None] * N_PAIR + near_column[:, 0].reshape(devices_all, BLK_G)) * PAIR_DEV + near_pair.reshape(devices_all, BLK_G)
    sources = jnp.concatenate([far_source, near_source], axis=1).astype(jnp.int32)
    targets = jnp.concatenate([far_target.reshape(devices_all, BLK_O), near_target.reshape(devices_all, BLK_G)], axis=1).astype(jnp.int32)
    for sweep_index in range(ITERS):
        rounded = current.astype(jnp.bfloat16)

        def one_device(device):
            margins = jnp.concatenate([lax.dynamic_slice_in_dim(far_margins, (device * BLK_O).astype(jnp.int32), BLK_O, 0), lax.dynamic_slice_in_dim(near_margins, (device * BLK_G).astype(jnp.int32), BLK_G, 0)], axis=0)
            source_blocks = rounded[sources[device]]
            halfway = batched(margins, source_blocks, "bij,bjk->bik").astype(jnp.bfloat16)
            contrib = batched(halfway, margins, "bik,blk->bil").astype(jnp.bfloat16)
            selector = (targets[device][None, :] == jnp.arange(PAIR_DEV, dtype=jnp.int32)[:, None]).astype(jnp.float32)
            return jnp.einsum("pb,bil->pil", selector, contrib.astype(jnp.float32))

        couple = lax.map(one_device, device_numbers).reshape(NPAIRS, P_SIZE, P_SIZE)
        fock_side = batched(fock_off, rounded, "pij,pjk->pik") + batched(rounded, fock_off, "pij,pkj->pik")
        inner_term = batched(rounded, exchange_ints, "pij,pjk->pik").astype(jnp.bfloat16)
        quadratic = batched(inner_term, rounded, "pij,pjk->pik") / P_SIZE
        residual = exchange_ints.astype(jnp.float32) + denominator * current + fock_side + couple + quadratic
        current = current - residual / denominator
    return current
```

```python
import functools
import math

import jax
import jax.numpy as jnp
from jax import lax
from jax.experimental import pallas as pl
from jax.experimental.pallas import tpu as pltpu
from jax.sharding import PartitionSpec as P

MESH = pl.DeviceIdType.MESH
SIZE = 128
PAIRS = 8
STRIDE = 16
F32 = jnp.float32
BF16 = jnp.bfloat16

ROW_PAIR, ROW_ORDER, ROW_BOUND, ROW_INDEX, NEAR_ORDER, NEAR_SOURCE, NEAR_BOUND = range(7)


def column(row):
    n = row.shape[1]
    diagonal = lax.broadcasted_iota(jnp.int32, (n, n), 0) == lax.broadcasted_iota(
        jnp.int32, (n, n), 1
    )
    return jnp.sum(jnp.where(diagonal, jnp.broadcast_to(row, (n, n)), 0.0), axis=1, keepdims=True)


def plan_kernel(ring, far_ref, near_ref, plan_ref):
    core = lax.rem(lax.axis_index("pair"), 2)
    group = far_ref[0:1, :]
    blocks = group.shape[1]
    shift = ring.bit_length() - 1
    high = lax.shift_right_logical(group, shift)
    low = jnp.bitwise_and(group, ring - 1)
    first = jnp.where(core == 0, high, low).astype(F32)
    second = jnp.where(core == 0, low, high).astype(F32)
    group = group.astype(F32)
    pair = far_ref[1:2, :].astype(F32)
    target = far_ref[2:3, :].astype(F32)
    group_c, first_c, second_c = column(group), column(first), column(second)
    pair_c, target_c = column(pair), column(target)
    here = lax.broadcasted_iota(jnp.int32, (blocks, blocks), 0)
    there = lax.broadcasted_iota(jnp.int32, (blocks, blocks), 1)
    earlier = there < here

    def count(mask):
        return jnp.sum(jnp.where(mask, 1.0, 0.0), axis=1, keepdims=True)

    twin = count((group_c == group) & earlier)
    place = second_c * 2.0 + twin
    slot = first_c * STRIDE + place
    smaller = (target < target_c) | ((target == target_c) & earlier)
    rank = count((first_c == first) & smaller)
    lane = lax.broadcasted_iota(jnp.int32, (blocks, SIZE), 1)
    lane_f = lane.astype(F32)
    number = lax.broadcasted_iota(jnp.int32, (blocks, SIZE), 0).astype(F32)

    def spread(where, value):
        return jnp.sum(jnp.where(where, value, 0.0), axis=0, keepdims=True)

    rows = [
        spread(slot == lane_f, jnp.broadcast_to(pair_c, lane.shape)),
        spread(first_c * STRIDE + rank == lane_f, jnp.broadcast_to(place, lane.shape)),
        spread(
            (first_c == lax.shift_right_logical(lane, 4).astype(F32))
            & (target_c < jnp.bitwise_and(lane, STRIDE - 1).astype(F32)),
            jnp.ones_like(lane_f),
        ),
        spread(slot == lane_f, number),
    ]

    near = near_ref[0:1, :].shape[1]
    source = near_ref[0:1, :].astype(F32) * PAIRS + near_ref[1:2, :].astype(F32)
    goal = near_ref[2:3, :].astype(F32)
    source_c, goal_c = column(source), column(goal)
    before = lax.broadcasted_iota(jnp.int32, (near, near), 1) < lax.broadcasted_iota(
        jnp.int32, (near, near), 0
    )
    near_rank = count((goal < goal_c) | ((goal == goal_c) & before))
    lanes = lax.broadcasted_iota(jnp.int32, (near, SIZE), 1).astype(F32)
    numbers = lax.broadcasted_iota(jnp.int32, (near, SIZE), 0).astype(F32)
    rows += [
        spread(near_rank == lanes, numbers),
        spread(near_rank == lanes, jnp.broadcast_to(source_c, lanes.shape)),
        spread(goal_c < lanes, jnp.ones_like(lanes)),
        jnp.zeros((1, SIZE), F32),
    ]
    for number_of, row in enumerate(rows):
        plan_ref[number_of : number_of + 1, :] = row.astype(jnp.int32)


def contribution(margin, source):
    halfway = jnp.dot(margin, source, preferred_element_type=F32).astype(BF16)
    return lax.dot_general(
        halfway, margin, (((1,), (1,)), ((), ())), preferred_element_type=F32
    ).astype(BF16)


def main_kernel(
    ring,
    columns,
    plan_ref,
    plan_smem,
    amplitudes,
    exchange,
    fock,
    energies,
    shift,
    far,
    near,
    out,
    margins_out,
    margins_in,
    plan_in,
    plans,
    gathered,
    rounded,
    later,
    near_one,
    near_two,
    contrib,
    prefix,
    near_prefix,
    denominator,
    partial_residual,
    state,
    sum_out,
    sum_in,
    margin_sem,
    plan_sem,
    plan_local_sem,
    gather_sem,
    near_sem,
    sum_sem,
):
    half_ring = ring // 2
    half = PAIRS // 2
    orb = lax.axis_index("orb")
    pair = lax.axis_index("pair")
    core = lax.rem(pair, 2)
    x = lax.div(pair, 2)
    high, low = lax.div(orb, ring), lax.rem(orb, ring)
    a = high * (1 - core) + low * core
    b = low * (1 - core) + high * core

    def along_a(step):
        return orb_of(lax.rem(a + (step % ring), ring), b)

    def along_b(step):
        return orb_of(a, lax.rem(b + (step % ring), ring))

    def orb_of(at_a, at_b):
        return (at_a * ring + at_b) * (1 - core) + (at_b * ring + at_a) * core

    def column_of(step):
        return lax.rem(x + (step % columns), columns) * 2 + core

    partner = x * 2 + 1 - core
    sends = []

    def send(src, dst, send_sem, recv_sem, device):
        copy = pltpu.make_async_remote_copy(
            src_ref=src,
            dst_ref=dst,
            send_sem=send_sem,
            recv_sem=recv_sem,
            device_id=device,
            device_id_type=MESH,
        )
        copy.start()
        sends.append(copy)

    def arrived(ref, sem):
        pltpu.make_async_copy(ref, ref, sem).wait()

    barrier = pltpu.get_barrier_semaphore()
    peers = [(along_a(d), pair) for d in range(1, ring)]
    peers += [(along_b(1), pair), (along_b(-1), pair)]
    peers += [(orb, column_of(e)) for e in range(1, columns)]
    peers += [(orb, partner)]
    for peer in peers:
        pl.semaphore_signal(barrier, inc=1, device_id=peer, device_id_type=MESH)

    order = [half_ring]
    for d in range(half_ring - 1, 0, -1):
        order += [d, ring - d]

    def collect(k, destination):
        goal = lax.rem(a + k, ring)

        def one(j, _):
            index = plan_smem[ROW_INDEX, goal * STRIDE + j]
            destination[j] = far[index]
            return 0

        lax.fori_loop(0, 2 * ring, one, 0, unroll=4)

    collect(order[0], margins_out.at[order[0]])
    pl.semaphore_wait(barrier, len(peers))

    def gather_start(turn, own, slots, distance_half):
        for h in range(2):
            part = pl.ds(h * half, half)
            gather_send(turn, own, slots, 1, h, part)

    def gather_send(turn, source, slots, level, h, part, ways=(0, 1)):
        for way in ways:
            if level == half_ring and h != way:
                continue
            number = level if (way == 0 or level == half_ring) else ring - level
            send(
                source.at[part],
                slots[number].at[part],
                gather_sem.at[0, turn, number, h],
                gather_sem.at[1, turn, number, h],
                (along_b(1 if way == 0 else -1), pair),
            )

    def gather_pass(turn, slots, level, h):
        part = pl.ds(h * half, half)
        for way in range(2):
            if level == half_ring:
                if h == way:
                    arrived(slots[level].at[part], gather_sem.at[1, turn, level, h])
                continue
            number = level if way == 0 else ring - level
            arrived(slots[number].at[part], gather_sem.at[1, turn, number, h])
            gather_send(turn, slots[number], slots, level + 1, h, part, (way,))

    def near_rows(at):
        return pl.ds(pl.multiple_of(at * PAIRS, PAIRS), PAIRS)

    def near_start(turn, own, slots):
        for e in range(1, columns):
            send(
                own,
                slots.at[near_rows(pair)],
                near_sem.at[0, turn, e],
                near_sem.at[1, turn, e],
                (orb, column_of(e)),
            )
        send(
            own,
            slots.at[near_rows(pair)],
            near_sem.at[0, turn, columns],
            near_sem.at[1, turn, columns],
            (orb, partner),
        )
        slots[near_rows(pair)] = own[...]

    def near_pass(turn, slots):
        for e in range(1, columns):
            rows = slots.at[near_rows(column_of(-e))]
            arrived(rows, near_sem.at[1, turn, e])
            send(
                rows,
                rows,
                near_sem.at[0, turn, columns + e],
                near_sem.at[1, turn, columns + e],
                (orb, partner),
            )

    def near_finish(turn, slots):
        for e in range(columns):
            came = lax.rem(x + columns - e, columns) * 2 + 1 - core
            arrived(slots.at[near_rows(came)], near_sem.at[1, turn, columns + e])
        blocks = near.shape[0]
        near_prefix[0] = jnp.zeros((SIZE, SIZE), F32)

        def one(k, total):
            margin = near[plan_smem[NEAR_ORDER, k]]
            total = total + contribution(margin, slots[plan_smem[NEAR_SOURCE, k]]).astype(F32)
            near_prefix[k + 1] = total
            return total

        lax.fori_loop(0, blocks, one, jnp.zeros((SIZE, SIZE), F32), unroll=2)

    def local_terms(current, source):
        def one(g, _):
            own = source[g]
            side = jnp.dot(fock[g], own, preferred_element_type=F32) + lax.dot_general(
                own, fock[g], (((1,), (1,)), ((), ())), preferred_element_type=F32
            )
            inner = jnp.dot(own, exchange[g], preferred_element_type=F32).astype(BF16)
            quadratic = jnp.dot(inner, own, preferred_element_type=F32) * (1.0 / SIZE)
            partial_residual[g] = (
                exchange[g].astype(F32)
                + denominator[g] * current[g].astype(F32)
                + side
                + quadratic
            )
            return 0

        lax.fori_loop(0, PAIRS, one, 0)

    def blocks_of(k, g, pairs_ref):
        origin = lax.rem(b + ring - g, ring)
        for twin in range(2):
            place = origin * 2 + twin
            index = plans[k, ROW_PAIR, a * STRIDE + place]
            contrib[k, place] = contribution(margins_in[k, place], pairs_ref(index))

    def prefixes(k):
        prefix[0] = jnp.zeros((SIZE, SIZE), F32)

        def one(j, total):
            total = total + contrib[k, plans[k, ROW_ORDER, a * STRIDE + j]].astype(F32)
            prefix[j + 1] = total
            return total

        lax.fori_loop(0, 2 * ring, one, jnp.zeros((SIZE, SIZE), F32), unroll=4)

    def share(k, t):
        start = plans[k, ROW_BOUND, a * STRIDE + t]
        stop = plans[k, ROW_BOUND, a * STRIDE + t + 1]
        return prefix[stop] - prefix[start]

    def near_share(t):
        start = plan_smem[NEAR_BOUND, t]
        stop = plan_smem[NEAR_BOUND, t + 1]
        return near_prefix[stop] - near_prefix[start]

    def has_input(way, level, h):
        return level + 1 < half_ring or (level + 1 == half_ring and h == way)

    def reduce_send(turn, way, level, k):
        for h in range(2):
            if level == half_ring and h != way:
                continue
            part = pl.ds(h * half, half)
            takes = has_input(way, level, h)
            incoming = sum_in.at[turn, way, level]
            outgoing = sum_out.at[turn, way, level - 1]
            if takes:
                arrived(incoming.at[part], sum_sem.at[1, turn, way, level, h])

            def one(i, _):
                t = h * half + i
                value = share(k, t)
                if takes:
                    value = value + incoming[t].astype(F32)
                outgoing[t] = value.astype(BF16)
                return 0

            lax.fori_loop(0, half, one, 0)
            send(
                outgoing.at[part],
                sum_in.at[turn, way, level - 1].at[part],
                sum_sem.at[0, turn, way, level - 1, h],
                sum_sem.at[1, turn, way, level - 1, h],
                (along_a(1 if way == 0 else -1), pair),
            )

    def reduce_level(turn, level):
        if level == half_ring:
            prefixes(half_ring)
            reduce_send(turn, 0, level, half_ring)
            reduce_send(turn, 1, level, half_ring)
        else:
            prefixes(ring - level)
            reduce_send(turn, 0, level, ring - level)
            prefixes(level)
            reduce_send(turn, 1, level, level)

    def update(turn, current, result):
        prefixes(0)
        for h in range(2):
            part = pl.ds(h * half, half)
            takes = [has_input(way, 0, h) for way in range(2)]
            for way in range(2):
                if takes[way]:
                    arrived(
                        sum_in.at[turn, way, 0].at[part], sum_sem.at[1, turn, way, 0, h]
                    )

            def one(i, _):
                t = h * half + i
                couple = share(0, t) + near_share(t)
                for way in range(2):
                    if takes[way]:
                        couple = couple + sum_in[turn, way, 0, t].astype(F32)
                residual = partial_residual[t] + couple
                new = current[t].astype(F32) - residual / denominator[t]
                result[t] = new
                if turn == 0:
                    rounded[t] = new.astype(BF16)
                return 0

            lax.fori_loop(0, half, one, 0)

    def margin_send(k):
        send(
            plan_ref,
            plan_in.at[k],
            plan_sem.at[0, k],
            plan_sem.at[1, k],
            (along_a(k), pair),
        )
        send(
            margins_out.at[k],
            margins_in.at[k],
            margin_sem.at[0, k],
            margin_sem.at[1, k],
            (along_a(k), pair),
        )

    slots_one = [gathered.at[g] for g in range(ring)]
    slots_two = [rounded] + list(later)
    margin_send(order[0])
    gather_start(0, amplitudes, slots_one, None)
    near_start(0, amplitudes, near_one)
    for k in order[1:]:
        collect(k, margins_out.at[k])
        margin_send(k)
    collect(0, margins_in.at[0])
    gathered[0] = amplitudes[...]
    own_plan = pltpu.make_async_copy(plan_ref, plans.at[0], plan_local_sem.at[0])
    own_plan.start()

    def denominators(g, _):
        row = jnp.broadcast_to(energies[pl.ds(g, 1), :], (SIZE, SIZE))
        denominator[g] = row + row.T + shift[0, g]
        return 0

    lax.fori_loop(0, PAIRS, denominators, 0)
    own_plan.wait()
    for level in range(1, half_ring + 1):
        for h in range(2):
            gather_pass(0, slots_one, level, h)
    local_terms(amplitudes, amplitudes)
    near_pass(0, near_one)
    near_finish(0, near_one)

    def all_groups(k):
        def one(g, _):
            blocks_of(k, g, lambda index: gathered[g, index])
            return 0

        lax.fori_loop(0, ring, one, 0, unroll=2)

    for level in range(half_ring, -1, -1):
        for k in [half_ring] if level == half_ring else [ring - level, level] if level else [0]:
            if k:
                arrived(plan_in.at[k], plan_sem.at[1, k])
                copy = pltpu.make_async_copy(plan_in.at[k], plans.at[k], plan_local_sem.at[k])
                copy.start()
                copy.wait()
                arrived(margins_in.at[k], margin_sem.at[1, k])
            all_groups(k)
        if level:
            reduce_level(0, level)
    update(0, amplitudes, state)

    gather_start(1, rounded, slots_two, None)
    near_start(1, rounded, near_two)

    def group(g):
        def one(k, _):
            blocks_of(k, g, lambda index: slots_two[g][index])
            return 0

        lax.fori_loop(0, ring, one, 0, unroll=2)

    group(0)
    local_terms(state, rounded)
    for level in range(1, half_ring + 1):
        for h in range(2):
            gather_pass(1, slots_two, level, h)
        group(level)
        if level != half_ring:
            group(ring - level)
    near_pass(1, near_two)
    for level in range(half_ring, 0, -1):
        reduce_level(1, level)
        if level == half_ring:
            near_finish(1, near_two)
    update(1, state, out)
    for copy in sends:
        copy.wait_send()


def on_device(
    amplitudes,
    exchange_ints,
    fock_off,
    orbital_energies,
    occ_shift,
    far_margins,
    far_group,
    far_pair,
    far_target,
    near_margins,
    near_column,
    near_pair,
    near_target,
):
    orb_count = lax.axis_size("orb")
    columns = lax.axis_size("pair") // 2
    ring = math.isqrt(orb_count)
    half_ring = ring // 2
    blocks, near_blocks = far_margins.shape[0], near_margins.shape[0]
    vmem = pl.BlockSpec(memory_space=pltpu.VMEM)
    smem = pl.BlockSpec(memory_space=pltpu.SMEM)
    far_table = jnp.stack([far_group[:, 0], far_pair, far_target])
    near_table = jnp.stack([near_column[:, 0], near_pair, near_target])
    plan = pl.pallas_call(
        functools.partial(plan_kernel, ring),
        out_shape=jax.ShapeDtypeStruct((8, SIZE), jnp.int32),
        in_specs=[vmem, vmem],
        out_specs=vmem,
    )(far_table, near_table)
    block = (SIZE, SIZE)
    owned = (PAIRS,) + block
    return pl.pallas_call(
        functools.partial(main_kernel, ring, columns),
        out_shape=jax.ShapeDtypeStruct(owned, F32),
        in_specs=[vmem, smem, vmem, vmem, vmem, vmem, smem, vmem, vmem],
        out_specs=vmem,
        scratch_shapes=[
            pltpu.VMEM((ring, 2 * ring) + block, BF16),
            pltpu.VMEM((ring, 2 * ring) + block, BF16),
            pltpu.VMEM((ring, 8, SIZE), jnp.int32),
            pltpu.SMEM((ring, 8, SIZE), jnp.int32),
            pltpu.VMEM((ring,) + owned, BF16),
            pltpu.VMEM(owned, BF16),
            [pltpu.VMEM(owned, BF16) for _ in range(ring - 1)],
            pltpu.VMEM((2 * columns * PAIRS,) + block, BF16),
            pltpu.VMEM((2 * columns * PAIRS,) + block, BF16),
            pltpu.VMEM((ring, 2 * ring) + block, BF16),
            pltpu.VMEM((2 * ring + 1,) + block, F32),
            pltpu.VMEM((near_blocks + 1,) + block, F32),
            pltpu.VMEM(owned, F32),
            pltpu.VMEM(owned, F32),
            pltpu.VMEM(owned, F32),
            pltpu.VMEM((2, 2, half_ring) + owned, BF16),
            pltpu.VMEM((2, 2, half_ring) + owned, BF16),
            pltpu.SemaphoreType.DMA((2, ring)),
            pltpu.SemaphoreType.DMA((2, ring)),
            pltpu.SemaphoreType.DMA((ring,)),
            pltpu.SemaphoreType.DMA((2, 2, ring, 2)),
            pltpu.SemaphoreType.DMA((2, 2, 2 * columns)),
            pltpu.SemaphoreType.DMA((2, 2, 2, half_ring, 2)),
        ],
        compiler_params=pltpu.CompilerParams(
            collective_id=0, has_side_effects=True, vmem_limit_bytes=60 * 1024 * 1024
        ),
    )(
        plan,
        plan,
        amplitudes,
        exchange_ints,
        fock_off,
        orbital_energies,
        occ_shift.reshape(1, PAIRS),
        far_margins,
        near_margins,
    )


def solution(mesh):
    placed = (
        P(("orb", "pair"), None, None),
        P(("orb", "pair"), None, None),
        P(("orb", "pair"), None, None),
        P(("orb", "pair"), None),
        P(("orb", "pair")),
        P(("orb", "pair"), None, None),
        P(("orb", "pair"), None),
        P(("orb", "pair")),
        P(("orb", "pair")),
        P(("orb", "pair"), None, None),
        P(("orb", "pair"), None),
        P(("orb", "pair")),
        P(("orb", "pair")),
    )
    return jax.shard_map(
        on_device,
        mesh=mesh,
        in_specs=placed,
        out_specs=P(("orb", "pair"), None, None),
        check_vma=False,
    )
```

```python
import functools
import math

import jax
import jax.numpy as jnp
from jax import lax
from jax.experimental import pallas as pl
from jax.experimental.pallas import tpu as pltpu
from jax.sharding import PartitionSpec as P

MESH = pl.DeviceIdType.MESH
SIZE = 128
PAIRS = 8
CHUNKS = 4
CHUNK = PAIRS // CHUNKS
STRIDE = 16
F32 = jnp.float32
BF16 = jnp.bfloat16

ROW_PAIR, ROW_ORDER, ROW_BOUND, ROW_INDEX, NEAR_ORDER, NEAR_SOURCE, NEAR_BOUND = range(7)


def column(row):
    n = row.shape[1]
    diagonal = lax.broadcasted_iota(jnp.int32, (n, n), 0) == lax.broadcasted_iota(
        jnp.int32, (n, n), 1
    )
    return jnp.sum(jnp.where(diagonal, jnp.broadcast_to(row, (n, n)), 0.0), axis=1, keepdims=True)


def plan_kernel(
    ring, group_ref, pair_ref, target_ref, column_ref, near_pair_ref, near_target_ref, plan_ref
):
    core = lax.rem(lax.axis_index("pair"), 2)
    group = group_ref[...]
    blocks = group.shape[1]
    shift = ring.bit_length() - 1
    high = lax.shift_right_logical(group, shift)
    low = jnp.bitwise_and(group, ring - 1)
    first = jnp.where(core == 0, high, low).astype(F32)
    second = jnp.where(core == 0, low, high).astype(F32)
    group = group.astype(F32)
    pair = pair_ref[...].astype(F32)
    target = target_ref[...].astype(F32)
    group_c, first_c, second_c = column(group), column(first), column(second)
    pair_c, target_c = column(pair), column(target)
    here = lax.broadcasted_iota(jnp.int32, (blocks, blocks), 0)
    there = lax.broadcasted_iota(jnp.int32, (blocks, blocks), 1)
    earlier = there < here

    def count(mask):
        return jnp.sum(jnp.where(mask, 1.0, 0.0), axis=1, keepdims=True)

    twin = count((group_c == group) & earlier)
    place = second_c * 2.0 + twin
    slot = first_c * STRIDE + place
    smaller = (target < target_c) | ((target == target_c) & earlier)
    rank = count((first_c == first) & smaller)
    lane = lax.broadcasted_iota(jnp.int32, (blocks, SIZE), 1)
    lane_f = lane.astype(F32)
    number = lax.broadcasted_iota(jnp.int32, (blocks, SIZE), 0).astype(F32)

    def spread(where, value):
        return jnp.sum(jnp.where(where, value, 0.0), axis=0, keepdims=True)

    rows = [
        spread(slot == lane_f, jnp.broadcast_to(pair_c, lane.shape)),
        spread(first_c * STRIDE + rank == lane_f, jnp.broadcast_to(place, lane.shape)),
        spread(
            (first_c == lax.shift_right_logical(lane, 4).astype(F32))
            & (target_c < jnp.bitwise_and(lane, STRIDE - 1).astype(F32)),
            jnp.ones_like(lane_f),
        ),
        spread(slot == lane_f, number),
    ]

    near = column_ref.shape[1]
    source = column_ref[...].astype(F32) * PAIRS + near_pair_ref[...].astype(F32)
    goal = near_target_ref[...].astype(F32)
    source_c, goal_c = column(source), column(goal)
    before = lax.broadcasted_iota(jnp.int32, (near, near), 1) < lax.broadcasted_iota(
        jnp.int32, (near, near), 0
    )
    near_rank = count((goal < goal_c) | ((goal == goal_c) & before))
    lanes = lax.broadcasted_iota(jnp.int32, (near, SIZE), 1).astype(F32)
    numbers = lax.broadcasted_iota(jnp.int32, (near, SIZE), 0).astype(F32)
    rows += [
        spread(near_rank == lanes, numbers),
        spread(near_rank == lanes, jnp.broadcast_to(source_c, lanes.shape)),
        spread(goal_c < lanes, jnp.ones_like(lanes)),
        jnp.zeros((1, SIZE), F32),
    ]
    for number_of, row in enumerate(rows):
        plan_ref[number_of : number_of + 1, :] = row.astype(jnp.int32)


def contribution(margin, source):
    halfway = jnp.dot(margin, source, preferred_element_type=F32).astype(BF16)
    return lax.dot_general(
        halfway, margin, (((1,), (1,)), ((), ())), preferred_element_type=F32
    ).astype(BF16)


def main_kernel(
    ring,
    columns,
    plan_ref,
    plan_smem,
    amplitudes_hbm,
    exchange_hbm,
    fock_hbm,
    energies,
    shift,
    far_hbm,
    near_hbm,
    out,
    amplitudes,
    exchange,
    fock,
    far,
    near,
    margins_out,
    margins_in,
    plan_in,
    plans,
    gathered,
    rounded,
    later,
    near_one,
    near_two,
    contrib,
    prefix,
    near_prefix,
    denominator,
    partial_residual,
    state,
    sum_out,
    sum_in,
    load_sem,
    margin_sem,
    plan_sem,
    plan_local_sem,
    gather_sem,
    near_sem,
    sum_sem,
):
    half_ring = ring // 2
    orb = lax.axis_index("orb")
    pair = lax.axis_index("pair")
    core = lax.rem(pair, 2)
    x = lax.div(pair, 2)
    high, low = lax.div(orb, ring), lax.rem(orb, ring)
    a = high * (1 - core) + low * core
    b = low * (1 - core) + high * core

    def orb_of(at_a, at_b):
        return (at_a * ring + at_b) * (1 - core) + (at_b * ring + at_a) * core

    def along_a(step):
        return orb_of(lax.rem(a + (step % ring), ring), b)

    def along_b(step):
        return orb_of(a, lax.rem(b + (step % ring), ring))

    def column_of(step):
        return lax.rem(x + (step % columns), columns) * 2 + core

    partner = x * 2 + 1 - core

    def send(src, dst, send_sem, recv_sem, device):
        pltpu.make_async_remote_copy(
            src_ref=src,
            dst_ref=dst,
            send_sem=send_sem,
            recv_sem=recv_sem,
            device_id=device,
            device_id_type=MESH,
        ).start()

    def done(ref, sem):
        pltpu.make_async_copy(ref, ref, sem).wait()

    barrier = pltpu.get_barrier_semaphore()
    peers = [(along_a(d), pair) for d in range(1, ring)]
    peers += [(along_b(1), pair), (along_b(-1), pair)]
    peers += [(orb, column_of(e)) for e in range(1, columns)]
    peers += [(orb, partner)]
    for peer in peers:
        pl.semaphore_signal(barrier, inc=1, device_id=peer, device_id_type=MESH)
    loads = [
        pltpu.make_async_copy(source, target, load_sem.at[n])
        for n, (source, target) in enumerate(
            [
                (far_hbm, far),
                (amplitudes_hbm, amplitudes),
                (exchange_hbm, exchange),
                (fock_hbm, fock),
                (near_hbm, near),
            ]
        )
    ]
    for load in loads:
        load.start()

    def collect(k, destination):
        goal = lax.rem(a + k, ring)

        def one(j, _):
            index = plan_smem[ROW_INDEX, goal * STRIDE + j]
            destination[j] = far[index]
            return 0

        lax.fori_loop(0, 2 * ring, one, 0, unroll=4)

    def part(q):
        return pl.ds(q * CHUNK, CHUNK)

    def goes(way, q):
        return q < CHUNKS // 2 if way == 0 else q >= CHUNKS // 2

    def when(condition, body):
        if isinstance(condition, bool):
            if condition:
                body()
        else:
            pl.when(condition)(body)

    def gather_send(turn, source, slots, level, q, way):
        number = level if (way == 0 or level == half_ring) else ring - level

        def go():
            send(
                source.at[part(q)],
                slots[number].at[part(q)],
                gather_sem.at[0, turn, number, q],
                gather_sem.at[1, turn, number, q],
                (along_b(1 if way == 0 else -1), pair),
            )

        if level == half_ring:
            when(goes(way, q), go)
        else:
            go()

    def gather_pass(turn, slots, level, q):
        for way in range(2):
            number = level if way == 0 else ring - level
            done(slots[number].at[part(q)], gather_sem.at[1, turn, number, q])
            gather_send(turn, slots[number], slots, level + 1, q, way)

    def gather_levels(turn, slots, work):
        for level in range(1, half_ring):

            def one(q, _):
                gather_pass(turn, slots, level, q)
                work(level, q)
                return 0

            lax.fori_loop(0, CHUNKS, one, 0)

        def last(q, _):
            for at in (q, q + CHUNKS // 2):
                done(slots[half_ring].at[part(at)], gather_sem.at[1, turn, half_ring, at])
                work(half_ring, at)
            return 0

        lax.fori_loop(0, CHUNKS // 2, last, 0)

    def near_rows(at):
        return pl.ds(pl.multiple_of(at * PAIRS, PAIRS), PAIRS)

    def near_start(turn, own, slots):
        for e in range(1, columns):
            send(
                own,
                slots.at[near_rows(pair)],
                near_sem.at[0, turn, e],
                near_sem.at[1, turn, e],
                (orb, column_of(e)),
            )
        send(
            own,
            slots.at[near_rows(pair)],
            near_sem.at[0, turn, columns],
            near_sem.at[1, turn, columns],
            (orb, partner),
        )
        slots[near_rows(pair)] = own[...]

    def near_pass(turn, slots):
        for e in range(1, columns):
            rows = slots.at[near_rows(column_of(-e))]
            done(rows, near_sem.at[1, turn, e])
            send(
                rows,
                rows,
                near_sem.at[0, turn, columns + e],
                near_sem.at[1, turn, columns + e],
                (orb, partner),
            )

    def near_finish(turn, slots):
        for e in range(columns):
            came = lax.rem(x + columns - e, columns) * 2 + 1 - core
            done(slots.at[near_rows(came)], near_sem.at[1, turn, columns + e])
        blocks = near.shape[0]
        near_prefix[0] = jnp.zeros((SIZE, SIZE), F32)

        def one(k, total):
            margin = near[plan_smem[NEAR_ORDER, k]]
            total = total + contribution(margin, slots[plan_smem[NEAR_SOURCE, k]]).astype(F32)
            near_prefix[k + 1] = total
            return total

        lax.fori_loop(0, blocks, one, jnp.zeros((SIZE, SIZE), F32), unroll=4)

    def local_term(current, source, g):
        own = source[g]
        side = jnp.dot(fock[g], own, preferred_element_type=F32) + lax.dot_general(
            own, fock[g], (((1,), (1,)), ((), ())), preferred_element_type=F32
        )
        inner = jnp.dot(own, exchange[g], preferred_element_type=F32).astype(BF16)
        quadratic = jnp.dot(inner, own, preferred_element_type=F32) * (1.0 / SIZE)
        partial_residual[g] = (
            exchange[g].astype(F32)
            + denominator[g] * current[g].astype(F32)
            + side
            + quadratic
        )

    def block_of(k, place, source):
        index = plans[k, ROW_PAIR, a * STRIDE + place]
        contrib[k, place] = contribution(margins_in[k, place], source(index))

    def prefixes(k, bank):
        prefix[bank, 0] = jnp.zeros((SIZE, SIZE), F32)

        def one(j, total):
            total = total + contrib[k, plans[k, ROW_ORDER, a * STRIDE + j]].astype(F32)
            prefix[bank, j + 1] = total
            return total

        lax.fori_loop(0, 2 * ring, one, jnp.zeros((SIZE, SIZE), F32), unroll=4)

    def share(k, bank, t):
        start = plans[k, ROW_BOUND, a * STRIDE + t]
        stop = plans[k, ROW_BOUND, a * STRIDE + t + 1]
        return prefix[bank, stop] - prefix[bank, start]

    def near_share(t):
        start = plan_smem[NEAR_BOUND, t]
        stop = plan_smem[NEAR_BOUND, t + 1]
        return near_prefix[stop] - near_prefix[start]

    def incoming(turn, way, level, q):
        def go():
            done(sum_in.at[turn, way, level].at[part(q)], sum_sem.at[1, turn, way, level, q])

        if level + 1 < half_ring:
            go()
        elif level + 1 == half_ring:
            when(goes(way, q), go)

    def added(turn, way, level, q, t, value):
        if level + 1 > half_ring:
            return value
        more = value + sum_in[turn, way, level, t].astype(F32)
        if level + 1 < half_ring:
            return more
        return jnp.where(goes(way, q), more, value)

    def reduce_send(turn, way, level, k, bank, q):
        incoming(turn, way, level, q)
        for i in range(CHUNK):
            t = q * CHUNK + i
            value = added(turn, way, level, q, t, share(k, bank, t))
            sum_out[turn, way, level - 1, t] = value.astype(BF16)
        send(
            sum_out.at[turn, way, level - 1].at[part(q)],
            sum_in.at[turn, way, level - 1].at[part(q)],
            sum_sem.at[0, turn, way, level - 1, q],
            sum_sem.at[1, turn, way, level - 1, q],
            (along_a(1 if way == 0 else -1), pair),
        )

    def reduce_level(turn, level):
        if level == half_ring:
            prefixes(half_ring, 0)

            def one(q, _):
                reduce_send(turn, 0, level, half_ring, 0, q)
                reduce_send(turn, 1, level, half_ring, 0, q + CHUNKS // 2)
                return 0

            lax.fori_loop(0, CHUNKS // 2, one, 0)
        else:
            prefixes(ring - level, 0)
            prefixes(level, 1)

            def two(q, _):
                reduce_send(turn, 0, level, ring - level, 0, q)
                reduce_send(turn, 1, level, level, 1, q)
                return 0

            lax.fori_loop(0, CHUNKS, two, 0)

    def update(turn, current, result, after):
        prefixes(0, 0)

        def one(q, _):
            for way in range(2):
                incoming(turn, way, 0, q)
            for i in range(CHUNK):
                t = q * CHUNK + i
                couple = share(0, 0, t) + near_share(t)
                for way in range(2):
                    couple = added(turn, way, 0, q, t, couple)
                residual = partial_residual[t] + couple
                new = current[t].astype(F32) - residual / denominator[t]
                result[t] = new
                if turn == 0:
                    rounded[t] = new.astype(BF16)
            after(q)
            return 0

        lax.fori_loop(0, CHUNKS, one, 0)

    slots_one = [gathered.at[g] for g in range(ring)]
    slots_two = [rounded] + list(later)
    levels = [[half_ring]] + [[ring - d, d] for d in range(half_ring - 1, 0, -1)]
    halves = [pl.ds(h * ring, ring) for h in range(2)]

    def margin_send(k):
        for h in range(2):
            send(
                margins_out.at[k].at[halves[h]],
                margins_in.at[k].at[halves[h]],
                margin_sem.at[0, k, h],
                margin_sem.at[1, k, h],
                (along_a(k), pair),
            )

    loads[0].wait()
    collect(half_ring, margins_out.at[half_ring])
    pl.semaphore_wait(barrier, len(peers))
    for k in levels[0]:
        margin_send(k)
    loads[1].wait()
    for q in range(CHUNKS):
        for way in range(2):
            gather_send(0, amplitudes, slots_one, 1, q, way)
    for k in range(1, ring):
        send(plan_ref, plan_in.at[k], plan_sem.at[0, k], plan_sem.at[1, k], (along_a(k), pair))
    for group in levels[1:]:
        for k in group:
            collect(k, margins_out.at[k])
            if group is levels[1]:
                margin_send(k)
    near_start(0, amplitudes, near_one)
    collect(0, margins_in.at[0])
    gathered[0] = amplitudes[...]

    def denominators(g, _):
        row = jnp.broadcast_to(energies[pl.ds(g, 1), :], (SIZE, SIZE))
        denominator[g] = row + row.T + shift[0, g]
        return 0

    lax.fori_loop(0, PAIRS, denominators, 0)
    loads[2].wait()
    loads[3].wait()
    loads[4].wait()

    def first_work(level, q):
        if level == 1:
            for i in range(CHUNK):
                local_term(amplitudes, amplitudes, q * CHUNK + i)

    if half_ring == 1:
        for q in range(CHUNKS):
            first_work(1, q)
        gather_levels(0, slots_one, lambda level, q: None)
    else:
        gather_levels(0, slots_one, first_work)
    near_pass(0, near_one)
    copies = []
    for k in range(ring):
        if k:
            done(plan_in.at[k], plan_sem.at[1, k])
        copies.append(
            pltpu.make_async_copy(plan_in.at[k] if k else plan_ref, plans.at[k], plan_local_sem.at[k])
        )
        copies[-1].start()
    for copy in copies:
        copy.wait()

    def half_target(k, h):
        for i in range(half_ring):
            origin = h * half_ring + i
            g = lax.rem(b + ring - origin, ring)
            for twin in range(2):
                block_of(k, origin * 2 + twin, lambda index: gathered[g, index])

    def target(k):
        for h in range(2):
            if not isinstance(k, int) or k:
                done(margins_in.at[k].at[halves[h]], margin_sem.at[1, k, h])
            half_target(k, h)

    target(0)
    near_finish(0, near_one)
    for n, group in enumerate(levels):
        if len(group) == 1:
            target(group[0])
        else:
            level = group[1]
            lax.fori_loop(
                0, 2, lambda n, _: (target(ring - level - n * (ring - 2 * level)), 0)[1], 0
            )
        reduce_level(0, half_ring - n)
        if n + 2 < len(levels):
            for k in levels[n + 2]:
                margin_send(k)

    def spread(q):
        for way in range(2):
            gather_send(1, rounded, slots_two, 1, q, way)

    update(0, amplitudes, state, spread)

    near_start(1, rounded, near_two)
    share_of = ring // CHUNKS

    def blocks_at(g, k):
        origin = lax.rem(b + ring - g, ring)
        for twin in range(2):
            block_of(k, origin * 2 + twin, lambda index: slots_two[g][index])

    def second_work(level, q):
        if level == 1:
            for i in range(CHUNK):
                local_term(state, rounded, q * CHUNK + i)
        for i in range(share_of):
            k = q * share_of + i
            blocks_at(level - 1, k)
            if level > 1:
                blocks_at(ring - level + 1, k)

    gather_levels(1, slots_two, second_work)
    near_pass(1, near_two)
    for n, group in enumerate(levels):
        for k in group:
            blocks_at(half_ring, k)
        reduce_level(1, half_ring - n)
        if n == 0:
            near_finish(1, near_two)
    blocks_at(half_ring, 0)
    update(1, state, out, lambda q: None)

    for k in range(1, ring):
        done(plan_ref, plan_sem.at[0, k])
        for h in range(2):
            done(margins_out.at[k].at[halves[h]], margin_sem.at[0, k, h])
    for turn, slots, near_slots in ((0, slots_one, near_one), (1, slots_two, near_two)):
        for number in range(1, ring):
            for q in range(CHUNKS):
                done(slots[number].at[part(q)], gather_sem.at[0, turn, number, q])
        for e in range(1, 2 * columns):
            done(near_slots.at[pl.ds(0, PAIRS)], near_sem.at[0, turn, e])
        for way in range(2):
            for level in range(half_ring):
                for q in range(CHUNKS):
                    if level + 1 < half_ring or goes(way, q):
                        done(
                            sum_out.at[turn, way, level].at[part(q)],
                            sum_sem.at[0, turn, way, level, q],
                        )


def on_device(
    amplitudes,
    exchange_ints,
    fock_off,
    orbital_energies,
    occ_shift,
    far_margins,
    far_group,
    far_pair,
    far_target,
    near_margins,
    near_column,
    near_pair,
    near_target,
):
    orb_count = lax.axis_size("orb")
    columns = lax.axis_size("pair") // 2
    ring = math.isqrt(orb_count)
    half_ring = ring // 2
    blocks, near_blocks = far_margins.shape[0], near_margins.shape[0]
    vmem = pl.BlockSpec(memory_space=pltpu.VMEM)
    smem = pl.BlockSpec(memory_space=pltpu.SMEM)
    hbm = pl.BlockSpec(memory_space=pl.ANY)
    plan = pl.pallas_call(
        functools.partial(plan_kernel, ring),
        out_shape=jax.ShapeDtypeStruct((8, SIZE), jnp.int32),
        in_specs=[vmem] * 6,
        out_specs=vmem,
    )(
        far_group.reshape(1, blocks),
        far_pair.reshape(1, blocks),
        far_target.reshape(1, blocks),
        near_column.reshape(1, near_blocks),
        near_pair.reshape(1, near_blocks),
        near_target.reshape(1, near_blocks),
    )
    block = (SIZE, SIZE)
    owned = (PAIRS,) + block
    return pl.pallas_call(
        functools.partial(main_kernel, ring, columns),
        out_shape=jax.ShapeDtypeStruct(owned, F32),
        in_specs=[vmem, smem, hbm, hbm, hbm, vmem, smem, hbm, hbm],
        out_specs=vmem,
        scratch_shapes=[
            pltpu.VMEM(owned, BF16),
            pltpu.VMEM(owned, BF16),
            pltpu.VMEM(owned, BF16),
            pltpu.VMEM((blocks,) + block, BF16),
            pltpu.VMEM((near_blocks,) + block, BF16),
            pltpu.VMEM((ring, 2 * ring) + block, BF16),
            pltpu.VMEM((ring, 2 * ring) + block, BF16),
            pltpu.VMEM((ring, 8, SIZE), jnp.int32),
            pltpu.SMEM((ring, 8, SIZE), jnp.int32),
            pltpu.VMEM((ring,) + owned, BF16),
            pltpu.VMEM(owned, BF16),
            [pltpu.VMEM(owned, BF16) for _ in range(ring - 1)],
            pltpu.VMEM((2 * columns * PAIRS,) + block, BF16),
            pltpu.VMEM((2 * columns * PAIRS,) + block, BF16),
            pltpu.VMEM((ring, 2 * ring) + block, BF16),
            pltpu.VMEM((2, 2 * ring + 1) + block, F32),
            pltpu.VMEM((near_blocks + 1,) + block, F32),
            pltpu.VMEM(owned, F32),
            pltpu.VMEM(owned, F32),
            pltpu.VMEM(owned, F32),
            pltpu.VMEM((2, 2, half_ring) + owned, BF16),
            pltpu.VMEM((2, 2, half_ring) + owned, BF16),
            pltpu.SemaphoreType.DMA((5,)),
            pltpu.SemaphoreType.DMA((2, ring, 2)),
            pltpu.SemaphoreType.DMA((2, ring)),
            pltpu.SemaphoreType.DMA((ring,)),
            pltpu.SemaphoreType.DMA((2, 2, ring, CHUNKS)),
            pltpu.SemaphoreType.DMA((2, 2, 2 * columns)),
            pltpu.SemaphoreType.DMA((2, 2, 2, half_ring, CHUNKS)),
        ],
        compiler_params=pltpu.CompilerParams(
            collective_id=0, has_side_effects=True, vmem_limit_bytes=60 * 1024 * 1024
        ),
    )(
        plan,
        plan,
        amplitudes,
        exchange_ints,
        fock_off,
        orbital_energies,
        occ_shift.reshape(1, PAIRS),
        far_margins,
        near_margins,
    )


def solution(mesh):
    placed = (
        P(("orb", "pair"), None, None),
        P(("orb", "pair"), None, None),
        P(("orb", "pair"), None, None),
        P(("orb", "pair"), None),
        P(("orb", "pair")),
        P(("orb", "pair"), None, None),
        P(("orb", "pair"), None),
        P(("orb", "pair")),
        P(("orb", "pair")),
        P(("orb", "pair"), None, None),
        P(("orb", "pair"), None),
        P(("orb", "pair")),
        P(("orb", "pair")),
    )
    return jax.shard_map(
        on_device,
        mesh=mesh,
        in_specs=placed,
        out_specs=P(("orb", "pair"), None, None),
        check_vma=False,
    )
```

```python
import functools
import math

import jax
import jax.numpy as jnp
from jax import lax
from jax.experimental import pallas as pl
from jax.experimental.pallas import tpu as pltpu
from jax.sharding import PartitionSpec as P

MESH = pl.DeviceIdType.MESH
SIZE = 128
PAIRS = 8
CHUNKS = 4
CHUNK = PAIRS // CHUNKS
STRIDE = 16
F32 = jnp.float32
BF16 = jnp.bfloat16

ROW_PAIR, ROW_ORDER, ROW_BOUND, ROW_INDEX, NEAR_ORDER, NEAR_SOURCE, NEAR_BOUND = range(7)


def column(row):
    n = row.shape[1]
    diagonal = lax.broadcasted_iota(jnp.int32, (n, n), 0) == lax.broadcasted_iota(
        jnp.int32, (n, n), 1
    )
    return jnp.sum(jnp.where(diagonal, jnp.broadcast_to(row, (n, n)), 0.0), axis=1, keepdims=True)


def plan_kernel(
    ring, group_ref, pair_ref, target_ref, column_ref, near_pair_ref, near_target_ref, plan_ref
):
    core = lax.rem(lax.axis_index("pair"), 2)
    group = group_ref[...]
    blocks = group.shape[1]
    shift = ring.bit_length() - 1
    high = lax.shift_right_logical(group, shift)
    low = jnp.bitwise_and(group, ring - 1)
    first = jnp.where(core == 0, high, low).astype(F32)
    second = jnp.where(core == 0, low, high).astype(F32)
    group = group.astype(F32)
    pair = pair_ref[...].astype(F32)
    target = target_ref[...].astype(F32)
    group_c, first_c, second_c = column(group), column(first), column(second)
    pair_c, target_c = column(pair), column(target)
    here = lax.broadcasted_iota(jnp.int32, (blocks, blocks), 0)
    there = lax.broadcasted_iota(jnp.int32, (blocks, blocks), 1)
    earlier = there < here

    def count(mask):
        return jnp.sum(jnp.where(mask, 1.0, 0.0), axis=1, keepdims=True)

    twin = count((group_c == group) & earlier)
    place = second_c * 2.0 + twin
    slot = first_c * STRIDE + place
    smaller = (target < target_c) | ((target == target_c) & earlier)
    rank = count((first_c == first) & smaller)
    lane = lax.broadcasted_iota(jnp.int32, (blocks, SIZE), 1)
    lane_f = lane.astype(F32)
    number = lax.broadcasted_iota(jnp.int32, (blocks, SIZE), 0).astype(F32)

    def spread(where, value):
        return jnp.sum(jnp.where(where, value, 0.0), axis=0, keepdims=True)

    rows = [
        spread(slot == lane_f, jnp.broadcast_to(pair_c, lane.shape)),
        jnp.minimum(
            spread(first_c * STRIDE + rank == lane_f, jnp.broadcast_to(place, lane.shape)),
            2.0 * ring - 1.0,
        ),
        jnp.minimum(
            spread(
                (first_c == lax.shift_right_logical(lane, 4).astype(F32))
                & (target_c < jnp.bitwise_and(lane, STRIDE - 1).astype(F32)),
                jnp.ones_like(lane_f),
            ),
            2.0 * ring,
        ),
        spread(slot == lane_f, number),
    ]

    near = column_ref.shape[1]
    source = column_ref[...].astype(F32) * PAIRS + near_pair_ref[...].astype(F32)
    goal = near_target_ref[...].astype(F32)
    source_c, goal_c = column(source), column(goal)
    before = lax.broadcasted_iota(jnp.int32, (near, near), 1) < lax.broadcasted_iota(
        jnp.int32, (near, near), 0
    )
    near_rank = count((goal < goal_c) | ((goal == goal_c) & before))
    lanes = lax.broadcasted_iota(jnp.int32, (near, SIZE), 1).astype(F32)
    numbers = lax.broadcasted_iota(jnp.int32, (near, SIZE), 0).astype(F32)
    rows += [
        spread(near_rank == lanes, numbers),
        spread(near_rank == lanes, jnp.broadcast_to(source_c, lanes.shape)),
        spread(goal_c < lanes, jnp.ones_like(lanes)),
        jnp.zeros((1, SIZE), F32),
    ]
    for number_of, row in enumerate(rows):
        plan_ref[number_of : number_of + 1, :] = row.astype(jnp.int32)


def contribution(margin, source):
    halfway = jnp.dot(margin, source, preferred_element_type=F32).astype(BF16)
    return lax.dot_general(
        halfway, margin, (((1,), (1,)), ((), ())), preferred_element_type=F32
    ).astype(BF16)


def main_kernel(
    ring,
    columns,
    plan_ref,
    plan_smem,
    amplitudes_hbm,
    exchange_hbm,
    fock_hbm,
    energies,
    shift,
    far_hbm,
    near_hbm,
    out,
    amplitudes,
    exchange,
    fock,
    far,
    near,
    margins_out,
    margins_in,
    plan_in,
    plans,
    gathered,
    rounded,
    later,
    near_one,
    near_two,
    contrib,
    prefix,
    near_prefix,
    denominator,
    partial_residual,
    state,
    sum_out,
    sum_in,
    load_sem,
    margin_sem,
    plan_sem,
    plan_local_sem,
    gather_sem,
    near_sem,
    sum_sem,
):
    half_ring = ring // 2
    orb = lax.axis_index("orb")
    pair = lax.axis_index("pair")
    core = lax.rem(pair, 2)
    x = lax.div(pair, 2)
    high, low = lax.div(orb, ring), lax.rem(orb, ring)
    a = high * (1 - core) + low * core
    b = low * (1 - core) + high * core

    def orb_of(at_a, at_b):
        return (at_a * ring + at_b) * (1 - core) + (at_b * ring + at_a) * core

    def along_a(step):
        return orb_of(lax.rem(a + (step % ring), ring), b)

    def along_b(step):
        return orb_of(a, lax.rem(b + (step % ring), ring))

    def column_of(step):
        return lax.rem(x + (step % columns), columns) * 2 + core

    partner = x * 2 + 1 - core

    def send(src, dst, send_sem, recv_sem, device):
        pltpu.make_async_remote_copy(
            src_ref=src,
            dst_ref=dst,
            send_sem=send_sem,
            recv_sem=recv_sem,
            device_id=device,
            device_id_type=MESH,
        ).start()

    def done(ref, sem):
        pltpu.make_async_copy(ref, ref, sem).wait()

    barrier = pltpu.get_barrier_semaphore()
    peers = [(along_a(d), pair) for d in range(1, ring)]
    peers += [(along_b(step), pair) for step in (1, -1, 2, -2)]
    peers += [(orb, column_of(e)) for e in range(1, columns)]
    peers += [(orb, partner)]
    for peer in peers:
        pl.semaphore_signal(barrier, inc=1, device_id=peer, device_id_type=MESH)
    loads = [
        pltpu.make_async_copy(source, target, load_sem.at[n])
        for n, (source, target) in enumerate(
            [
                (far_hbm, far),
                (amplitudes_hbm, amplitudes),
                (exchange_hbm, exchange),
                (fock_hbm, fock),
                (near_hbm, near),
            ]
        )
    ]
    for load in loads:
        load.start()
    for load in loads:
        load.wait()

    def collect(k, destination):
        goal = lax.rem(a + k, ring)

        def one(j, _):
            index = plan_smem[ROW_INDEX, goal * STRIDE + j]
            destination[j] = far[index]
            return 0

        lax.fori_loop(0, 2 * ring, one, 0, unroll=4)

    def part(q):
        return pl.ds(q * CHUNK, CHUNK)

    def goes(way, q):
        return q < CHUNKS // 2 if way == 0 else q >= CHUNKS // 2

    def when(condition, body):
        if isinstance(condition, bool):
            if condition:
                body()
        else:
            pl.when(condition)(body)

    def gather_send(turn, source, slots, level, q, way):
        if level < half_ring:
            number = level if way == 0 else ring - level
            send(
                source.at[part(q)],
                slots[number].at[part(q)],
                gather_sem.at[0, turn, number, q],
                gather_sem.at[1, turn, number, q],
                (along_b(1 if way == 0 else -1), pair),
            )

        def opposite():
            send(
                source.at[part(q)],
                slots[half_ring].at[part(q)],
                gather_sem.at[0, turn, half_ring, q],
                gather_sem.at[1, turn, half_ring, q],
                (along_b(2 if way == 0 else -2), pair),
            )

        if level == half_ring - 1:
            when(goes(way, q), opposite)

    def gather_pass(turn, slots, level, q):
        for way in range(2):
            number = level if way == 0 else ring - level
            done(slots[number].at[part(q)], gather_sem.at[1, turn, number, q])
            gather_send(turn, slots[number], slots, level + 1, q, way)

    def gather_levels(turn, slots, work, between=None):
        for level in range(1, half_ring):
            if level == 2 and between is not None:
                between()

            def one(q, _):
                gather_pass(turn, slots, level, q)
                work(level, q)
                return 0

            lax.fori_loop(0, CHUNKS, one, 0)
        if half_ring == 2 and between is not None:
            between()

        def last(q, _):
            for at in (q, q + CHUNKS // 2):
                done(slots[half_ring].at[part(at)], gather_sem.at[1, turn, half_ring, at])
                work(half_ring, at)
            return 0

        lax.fori_loop(0, CHUNKS // 2, last, 0)

    def near_rows(at):
        return pl.ds(pl.multiple_of(at * PAIRS, PAIRS), PAIRS)

    def near_start(turn, own, slots):
        for e in range(1, columns):
            send(
                own,
                slots.at[near_rows(pair)],
                near_sem.at[0, turn, e],
                near_sem.at[1, turn, e],
                (orb, column_of(e)),
            )
        send(
            own,
            slots.at[near_rows(pair)],
            near_sem.at[0, turn, columns],
            near_sem.at[1, turn, columns],
            (orb, partner),
        )
        slots[near_rows(pair)] = own[...]

    def near_pass(turn, slots):
        for e in range(1, columns):
            rows = slots.at[near_rows(column_of(-e))]
            done(rows, near_sem.at[1, turn, e])
            send(
                rows,
                rows,
                near_sem.at[0, turn, columns + e],
                near_sem.at[1, turn, columns + e],
                (orb, partner),
            )

    def near_finish(turn, slots):
        for e in range(columns):
            came = lax.rem(x + columns - e, columns) * 2 + 1 - core
            done(slots.at[near_rows(came)], near_sem.at[1, turn, columns + e])
        blocks = near.shape[0]
        near_prefix[0] = jnp.zeros((SIZE, SIZE), F32)

        def one(k, total):
            margin = near[plan_smem[NEAR_ORDER, k]]
            total = total + contribution(margin, slots[plan_smem[NEAR_SOURCE, k]]).astype(F32)
            near_prefix[k + 1] = total
            return total

        lax.fori_loop(0, blocks, one, jnp.zeros((SIZE, SIZE), F32), unroll=4)

    def local_term(current, source, g):
        own = source[g]
        side = jnp.dot(fock[g], own, preferred_element_type=F32) + lax.dot_general(
            own, fock[g], (((1,), (1,)), ((), ())), preferred_element_type=F32
        )
        inner = jnp.dot(own, exchange[g], preferred_element_type=F32).astype(BF16)
        quadratic = jnp.dot(inner, own, preferred_element_type=F32) * (1.0 / SIZE)
        partial_residual[g] = (
            exchange[g].astype(F32)
            + denominator[g] * current[g].astype(F32)
            + side
            + quadratic
        )

    def block_of(k, place, source):
        index = plans[k, ROW_PAIR, a * STRIDE + place]
        contrib[k, place] = contribution(margins_in[k, place], source(index))

    def prefixes(k, bank):
        prefix[bank, 0] = jnp.zeros((SIZE, SIZE), F32)

        def one(j, total):
            total = total + contrib[k, plans[k, ROW_ORDER, a * STRIDE + j]].astype(F32)
            prefix[bank, j + 1] = total
            return total

        lax.fori_loop(0, 2 * ring, one, jnp.zeros((SIZE, SIZE), F32), unroll=4)

    def share(k, bank, t):
        start = plans[k, ROW_BOUND, a * STRIDE + t]
        stop = plans[k, ROW_BOUND, a * STRIDE + t + 1]
        return prefix[bank, stop] - prefix[bank, start]

    def near_share(t):
        start = plan_smem[NEAR_BOUND, t]
        stop = plan_smem[NEAR_BOUND, t + 1]
        return near_prefix[stop] - near_prefix[start]

    def incoming(turn, way, level, q):
        def wait(slot):
            done(sum_in.at[turn, way, slot].at[part(q)], sum_sem.at[1, turn, way, slot, q])

        if level < half_ring - 1:
            wait(level)
        if level == half_ring - 2:
            when(goes(way, q), lambda: wait(half_ring - 1))

    def added(turn, way, level, q, t, value):
        if level < half_ring - 1:
            value = value + sum_in[turn, way, level, t].astype(F32)
        if level == half_ring - 2:
            more = value + sum_in[turn, way, half_ring - 1, t].astype(F32)
            value = jnp.where(goes(way, q), more, value)
        return value

    def reduce_send(turn, way, level, k, bank, q):
        incoming(turn, way, level, q)
        for i in range(CHUNK):
            t = q * CHUNK + i
            value = added(turn, way, level, q, t, share(k, bank, t))
            sum_out[turn, way, level - 1, t] = value.astype(BF16)
        send(
            sum_out.at[turn, way, level - 1].at[part(q)],
            sum_in.at[turn, way, level - 1].at[part(q)],
            sum_sem.at[0, turn, way, level - 1, q],
            sum_sem.at[1, turn, way, level - 1, q],
            (along_a((2 if level == half_ring else 1) * (1 if way == 0 else -1)), pair),
        )

    def reduce_level(turn, level):
        if level == half_ring:
            prefixes(half_ring, 0)

            def one(q, _):
                reduce_send(turn, 0, level, half_ring, 0, q)
                reduce_send(turn, 1, level, half_ring, 0, q + CHUNKS // 2)
                return 0

            lax.fori_loop(0, CHUNKS // 2, one, 0)
        else:
            prefixes(ring - level, 0)
            prefixes(level, 1)

            def two(q, _):
                reduce_send(turn, 0, level, ring - level, 0, q)
                reduce_send(turn, 1, level, level, 1, q)
                return 0

            lax.fori_loop(0, CHUNKS, two, 0)

    def update(turn, current, result, after):
        prefixes(0, 0)

        def one(q, _):
            for way in range(2):
                incoming(turn, way, 0, q)
            for i in range(CHUNK):
                t = q * CHUNK + i
                couple = share(0, 0, t) + near_share(t)
                for way in range(2):
                    couple = added(turn, way, 0, q, t, couple)
                residual = partial_residual[t] + couple
                new = current[t].astype(F32) - residual / denominator[t]
                result[t] = new
                if turn == 0:
                    rounded[t] = new.astype(BF16)
            after(q)
            return 0

        lax.fori_loop(0, CHUNKS, one, 0)

    slots_one = [gathered.at[g] for g in range(ring)]
    slots_two = [rounded] + list(later)
    levels = [[half_ring]] + [[ring - d, d] for d in range(half_ring - 1, 0, -1)]
    halves = [pl.ds(h * ring, ring) for h in range(2)]

    def margin_send(k):
        for h in range(2):
            send(
                margins_out.at[k].at[halves[h]],
                margins_in.at[k].at[halves[h]],
                margin_sem.at[0, k, h],
                margin_sem.at[1, k, h],
                (along_a(k), pair),
            )

    collect(half_ring, margins_out.at[half_ring])
    pl.semaphore_wait(barrier, len(peers))
    for q in range(CHUNKS):
        for way in range(2):
            gather_send(0, amplitudes, slots_one, 1, q, way)
    for k in range(1, ring):
        send(plan_ref, plan_in.at[k], plan_sem.at[0, k], plan_sem.at[1, k], (along_a(k), pair))
    for group in levels[1:]:
        for k in group:
            collect(k, margins_out.at[k])
    near_start(0, amplitudes, near_one)
    collect(0, margins_in.at[0])
    gathered[0] = amplitudes[...]

    def denominators(g, _):
        row = jnp.broadcast_to(energies[pl.ds(g, 1), :], (SIZE, SIZE))
        denominator[g] = row + row.T + shift[0, g]
        return 0

    lax.fori_loop(0, PAIRS, denominators, 0)

    def margins_leave():
        for group in levels:
            for k in group:
                margin_send(k)

    def first_work(level, q):
        if level == 1:
            for i in range(CHUNK):
                local_term(amplitudes, amplitudes, q * CHUNK + i)

    gather_levels(0, slots_one, first_work, margins_leave)
    near_pass(0, near_one)
    copies = []
    for k in range(ring):
        if k:
            done(plan_in.at[k], plan_sem.at[1, k])
        copies.append(
            pltpu.make_async_copy(plan_in.at[k] if k else plan_ref, plans.at[k], plan_local_sem.at[k])
        )
        copies[-1].start()
    for copy in copies:
        copy.wait()

    def half_target(k, h):
        for i in range(half_ring):
            origin = h * half_ring + i
            g = lax.rem(b + ring - origin, ring)
            for twin in range(2):
                block_of(k, origin * 2 + twin, lambda index: gathered[g, index])

    def target(k):
        for h in range(2):
            if not isinstance(k, int) or k:
                done(margins_in.at[k].at[halves[h]], margin_sem.at[1, k, h])
            half_target(k, h)

    target(0)
    near_finish(0, near_one)
    for n, group in enumerate(levels):
        if len(group) == 1:
            target(group[0])
        else:
            level = group[1]
            lax.fori_loop(
                0, 2, lambda n, _: (target(ring - level - n * (ring - 2 * level)), 0)[1], 0
            )
        reduce_level(0, half_ring - n)

    def spread(q):
        for way in range(2):
            gather_send(1, rounded, slots_two, 1, q, way)

    update(0, amplitudes, state, spread)

    near_start(1, rounded, near_two)
    share_of = ring // CHUNKS

    def blocks_at(g, k):
        origin = lax.rem(b + ring - g, ring)
        for twin in range(2):
            block_of(k, origin * 2 + twin, lambda index: slots_two[g][index])

    def second_work(level, q):
        if level == 1:
            for i in range(CHUNK):
                local_term(state, rounded, q * CHUNK + i)
        for i in range(share_of):
            k = q * share_of + i
            blocks_at(level - 1, k)
            if level > 1:
                blocks_at(ring - level + 1, k)

    gather_levels(1, slots_two, second_work)
    near_pass(1, near_two)
    for n, group in enumerate(levels):
        for k in group:
            blocks_at(half_ring, k)
        reduce_level(1, half_ring - n)
        if n == 0:
            near_finish(1, near_two)
    blocks_at(half_ring, 0)
    update(1, state, out, lambda q: None)

    for k in range(1, ring):
        done(plan_ref, plan_sem.at[0, k])
        for h in range(2):
            done(margins_out.at[k].at[halves[h]], margin_sem.at[0, k, h])
    for turn, slots, near_slots in ((0, slots_one, near_one), (1, slots_two, near_two)):
        for number in range(1, ring):
            for q in range(CHUNKS):
                done(slots[number].at[part(q)], gather_sem.at[0, turn, number, q])
        for e in range(1, 2 * columns):
            done(near_slots.at[pl.ds(0, PAIRS)], near_sem.at[0, turn, e])
        for way in range(2):
            for level in range(half_ring):
                for q in range(CHUNKS):
                    if level + 1 < half_ring or goes(way, q):
                        done(
                            sum_out.at[turn, way, level].at[part(q)],
                            sum_sem.at[0, turn, way, level, q],
                        )


def on_device(
    amplitudes,
    exchange_ints,
    fock_off,
    orbital_energies,
    occ_shift,
    far_margins,
    far_group,
    far_pair,
    far_target,
    near_margins,
    near_column,
    near_pair,
    near_target,
):
    orb_count = lax.axis_size("orb")
    columns = lax.axis_size("pair") // 2
    ring = math.isqrt(orb_count)
    half_ring = ring // 2
    blocks, near_blocks = far_margins.shape[0], near_margins.shape[0]
    vmem = pl.BlockSpec(memory_space=pltpu.VMEM)
    smem = pl.BlockSpec(memory_space=pltpu.SMEM)
    hbm = pl.BlockSpec(memory_space=pl.ANY)
    tables = [
        far_group.reshape(1, blocks),
        far_pair.reshape(1, blocks),
        far_target.reshape(1, blocks),
        near_column.reshape(1, near_blocks),
        near_pair.reshape(1, near_blocks),
        near_target.reshape(1, near_blocks),
    ]
    plan = pl.pallas_call(
        functools.partial(plan_kernel, ring),
        out_shape=jax.ShapeDtypeStruct((8, SIZE), jnp.int32),
        in_specs=[vmem] * 6,
        out_specs=vmem,
    )(*tables)
    block = (SIZE, SIZE)
    owned = (PAIRS,) + block
    return pl.pallas_call(
        functools.partial(main_kernel, ring, columns),
        out_shape=jax.ShapeDtypeStruct(owned, F32),
        in_specs=[vmem, smem, hbm, hbm, hbm, vmem, smem, hbm, hbm],
        out_specs=vmem,
        scratch_shapes=[
            pltpu.VMEM(owned, BF16),
            pltpu.VMEM(owned, BF16),
            pltpu.VMEM(owned, BF16),
            pltpu.VMEM((blocks,) + block, BF16),
            pltpu.VMEM((near_blocks,) + block, BF16),
            pltpu.VMEM((ring, 2 * ring) + block, BF16),
            pltpu.VMEM((ring, 2 * ring) + block, BF16),
            pltpu.VMEM((ring, 8, SIZE), jnp.int32),
            pltpu.SMEM((ring, 8, SIZE), jnp.int32),
            pltpu.VMEM((ring,) + owned, BF16),
            pltpu.VMEM(owned, BF16),
            [pltpu.VMEM(owned, BF16) for _ in range(ring - 1)],
            pltpu.VMEM((2 * columns * PAIRS,) + block, BF16),
            pltpu.VMEM((2 * columns * PAIRS,) + block, BF16),
            pltpu.VMEM((ring, 2 * ring) + block, BF16),
            pltpu.VMEM((2, 2 * ring + 1) + block, F32),
            pltpu.VMEM((near_blocks + 1,) + block, F32),
            pltpu.VMEM(owned, F32),
            pltpu.VMEM(owned, F32),
            pltpu.VMEM(owned, F32),
            pltpu.VMEM((2, 2, half_ring) + owned, BF16),
            pltpu.VMEM((2, 2, half_ring) + owned, BF16),
            pltpu.SemaphoreType.DMA((5,)),
            pltpu.SemaphoreType.DMA((2, ring, 2)),
            pltpu.SemaphoreType.DMA((2, ring)),
            pltpu.SemaphoreType.DMA((ring,)),
            pltpu.SemaphoreType.DMA((2, 2, ring, CHUNKS)),
            pltpu.SemaphoreType.DMA((2, 2, 2 * columns)),
            pltpu.SemaphoreType.DMA((2, 2, 2, half_ring, CHUNKS)),
        ],
        compiler_params=pltpu.CompilerParams(
            collective_id=0, has_side_effects=True, vmem_limit_bytes=60 * 1024 * 1024
        ),
    )(
        plan,
        plan,
        amplitudes,
        exchange_ints,
        fock_off,
        orbital_energies,
        occ_shift.reshape(1, PAIRS),
        far_margins,
        near_margins,
    )


def solution(mesh):
    placed = (
        P(("orb", "pair"), None, None),
        P(("orb", "pair"), None, None),
        P(("orb", "pair"), None, None),
        P(("orb", "pair"), None),
        P(("orb", "pair")),
        P(("orb", "pair"), None, None),
        P(("orb", "pair"), None),
        P(("orb", "pair")),
        P(("orb", "pair")),
        P(("orb", "pair"), None, None),
        P(("orb", "pair"), None),
        P(("orb", "pair")),
        P(("orb", "pair")),
    )
    return jax.shard_map(
        on_device,
        mesh=mesh,
        in_specs=placed,
        out_specs=P(("orb", "pair"), None, None),
        check_vma=False,
    )
```
